32 devices in a mesh: dp: 8 (over z, y), section: 2 (over core), tensor: 2 (over x).
Axes of the slice: x: 2, y: 2, z: 4, core: 2. Of those that a mesh axis runs over, the one named last changes fastest.
Arguments:
- tower_input: bfloat16 [2, 1536, 1024], P('section', 'dp'), may hold values from -8 to 8
- up_weight: bfloat16 [2, 1024, 4096], P('section', None, 'tensor'), may hold values from -0.1875 to 0.1875
- down_weight: bfloat16 [2, 4096, 1024], P('section', 'tensor'), may hold values from -0.09375 to 0.09375
- pair: int32 [1536], P('dp'), may hold values from 0 to 1535, each once
- scale: float32 [1], replicated, may hold values from 4 to 16
- bias: float32 [1], replicated, may hold values from -4 to -1
Outputs:
- loss: float32 [1], replicated
- slide_grad: float32 [1536, 1024], P(('dp', 'section', 'tensor'))
- report_grad: float32 [1536, 1024], P(('dp', 'section', 'tensor'))
The draws below stay inside these ranges and needn't reach their ends.
Inputs may be any that keep to these rules, and one draw needn't show every extreme that they name: `pair`: each report index appears exactly once.
All inputs are finite; a program needn't handle non-finite values.
Results may differ from the reference program's by a relative error of at most 0.00036.
Values may be sent and summed in bfloat16 or wider, within the bound.
A program may use at most 128 MiB of HBM per device.

```python
import math
import jax
import jax.numpy as jnp
from jax import lax

D = 1024
H = 4096
PAIRS_DEV = 48
B = 1536


def draw_tower_input(key, part):
    key_center = jax.random.fold_in(key, 11)
    key_member = jax.random.fold_in(key, 12)
    key_strength = jax.random.fold_in(key, 13)
    key_noise = jax.random.fold_in(key, 14)
    groups = 8
    centers = jax.random.normal(key_center, (groups, D), jnp.float32)
    member = jax.random.randint(key_member, (2, B), 0, groups)
    strength = jnp.exp(jax.random.uniform(key_strength, (2, B, 1), jnp.float32, jnp.log(0.4), jnp.log(1.6)))
    noise = 0.6 * jax.random.normal(key_noise, (2, B, D), jnp.float32)
    shared = jnp.take(centers, member, axis=0) * strength
    values = jnp.clip(shared + noise, -8.0, 8.0)
    return values.astype(jnp.bfloat16)


def level_of(key, shape, split, least, top_value):
    factor_of, own = 1.0, jax.random.fold_in(key, 6)
    for dim, shards_of in split:
        heights = jnp.exp(jax.random.uniform(jax.random.fold_in(own, dim), (shards_of,), jnp.float32, least / len(split), top_value / len(split)))
        factor_of = factor_of * jnp.repeat(heights, shape[dim] // shards_of).reshape([-1 if axis == dim else 1 for axis in range(len(shape))])
    return factor_of


def scatter_about(rng, extent, scale, reach, split=(), kind=jnp.bfloat16):
    result = jax.random.normal(rng, extent, jnp.float32) * scale
    if len(split) > 0:
        result = level_of(rng, extent, split, -0.22, 0.18) * result
    return jnp.clip(result, min=-reach, max=reach).astype(kind)


def setup_inputs(seed: int = 0) -> dict:
    streams_of = jax.random.split(jax.random.key(seed), 7)
    return {
        "tower_input": draw_tower_input(jax.random.fold_in(streams_of[6], 71), 0),
        "up_weight": scatter_about(streams_of[1], (2, D, H), D ** -0.5, 0.1875, ((0, 2), (2, 2))),
        "down_weight": scatter_about(streams_of[2], (2, H, D), H ** -0.5, 0.09375, ((0, 2), (1, 2))),
        "pair": jax.random.permutation(streams_of[3], B).astype(jnp.int32),
        "scale": jnp.clip(jnp.exp(jax.random.uniform(streams_of[4], (1,), jnp.float32, math.log(4.0), math.log(16.0))), 4.0, 16.0),
        "bias": jnp.clip(jax.random.uniform(streams_of[5], (1,), jnp.float32, -4.0, -1.0), -4.0, -1.0),
    }


def tower(inputs, up_part, down_part):
    hidden = jax.nn.gelu(jnp.dot(inputs, up_part, preferred_element_type=jnp.float32)).astype(jnp.bfloat16)
    raw = inputs.astype(jnp.float32) + jnp.dot(hidden, down_part, preferred_element_type=jnp.float32)
    norms = lax.rsqrt(lax.optimization_barrier(jnp.sum(raw * raw, axis=-1, keepdims=True)) + 1e-06)
    return (raw * norms).astype(jnp.bfloat16)

def reference(tower_input, up_weight, down_weight, pair, scale, bias):
    slides = tower(tower_input[0], up_weight[0], down_weight[0])
    reports = tower(tower_input[1], up_weight[1], down_weight[1])
    total = slides.shape[0]
    block = 4 * PAIRS_DEV
    columns = jnp.arange(total, dtype=jnp.int32)

    def step(carry, index):
        loss_sum, report_sum = carry
        start = (index * block).astype(jnp.int32)
        slide_rows = lax.dynamic_slice_in_dim(slides, start, block, 0)
        pair_rows = lax.dynamic_slice_in_dim(pair, start, block, 0)
        logits = scale[0] * lax.dot_general(slide_rows, reports, (((1,), (1,)), ((), ())), preferred_element_type=jnp.float32) + bias[0]
        sign = jnp.where(pair_rows[:, None] == columns[None, :], 1.0, -1.0).astype(jnp.float32)
        loss_sum = loss_sum + jnp.sum(jnp.logaddexp(jnp.float32(0.0), -sign * logits))
        weight = (-scale[0] * sign * jax.nn.sigmoid(-sign * logits)).astype(jnp.bfloat16)
        slide_part = jnp.dot(weight, reports, preferred_element_type=jnp.float32)
        report_sum = report_sum + lax.dot_general(weight, slide_rows, (((0,), (0,)), ((), ())), preferred_element_type=jnp.float32)
        return ((loss_sum, report_sum), slide_part)
    start_carry = (jnp.zeros((), jnp.float32), jnp.zeros((total, D), jnp.float32))
    (loss_sum, report_grad), slide_parts = lax.scan(step, start_carry, jnp.arange(total // block, dtype=jnp.int32))
    loss = (loss_sum / total).reshape(1)
    return (loss, slide_parts.reshape(total, D), report_grad)
```

```python
import functools

import jax
import jax.numpy as jnp
from jax import lax
from jax.experimental import pallas as pl
from jax.experimental.pallas import tpu as pltpu
from jax.sharding import PartitionSpec as P

MESH = pl.DeviceIdType.MESH
INNER = 2
UP_PARTS = 4
DOWN_PARTS = 2
X, Y, ZM, ZP, CORE = range(5)


def wait_bytes(ref, sem):
    pltpu.make_async_copy(ref, ref, sem).wait()


def kernel(
    dims,
    scale_ref, bias_ref, left_ref, tile_ref, x_ref, up_ref, down_ref,
    loss_out, slide_out, report_out,
    xs, up, down, hid, part, recv, emb, got, tiles, grad, grad_in, loss_acc, loss_row, loss_all,
    x_sem, up_sem, down_sem, part_send, part_recv, own_send, fwd_send, got_recv,
    tile_send, tile_recv, grad_send, grad_recv, loss_send, loss_recv,
):
    n_dp, n_section, n_tensor, n_part, n_rows, width, total = dims
    n_outer = n_dp // INNER
    quarter = xs.shape[0] // (n_section * n_tensor)
    own_rows = n_section * quarter
    d, s, x = lax.axis_index("dp"), lax.axis_index("section"), lax.axis_index("tensor")
    z, y = d // INNER, lax.rem(d, INNER)
    ox, oy, os = 1 - x, 1 - y, 1 - s
    n_all = n_dp * n_section * n_tensor
    me = (d * n_section + s) * n_tensor + x

    def device(zz, yy, ss, xx):
        return {"dp": zz * INNER + yy, "section": ss, "tensor": xx}

    def device_of(n):
        return {
            "dp": n // (n_section * n_tensor),
            "section": lax.rem(n // n_tensor, n_section),
            "tensor": lax.rem(n, n_tensor),
        }

    x_copies = []
    for half, t in ((0, ox), (1, x)):
        for q in range(n_section):
            x_copies.append(pltpu.make_async_copy(
                x_ref.at[pl.ds(pl.multiple_of((q * n_tensor + t) * quarter, 16), quarter)],
                xs.at[pl.ds(half * own_rows + q * quarter, quarter)],
                x_sem.at[half * n_section + q],
            ))
    for c in x_copies:
        c.start()
    up_w = up.shape[1] // UP_PARTS
    down_w = down.shape[1] // DOWN_PARTS

    def up_copy(i):
        cols = pl.ds(pl.multiple_of(i * up_w, 128), up_w)
        return pltpu.make_async_copy(up_ref.at[:, cols], up.at[:, cols], up_sem.at[i])

    def down_copy(i):
        cols = pl.ds(pl.multiple_of(i * down_w, 128), down_w)
        return pltpu.make_async_copy(down_ref.at[:, cols], down.at[:, cols], down_sem.at[i])

    for i in range(UP_PARTS):
        up_copy(i).start()
    for i in range(DOWN_PARTS):
        down_copy(i).start()

    barrier = pltpu.get_barrier_semaphore()

    def greet(n, carry):
        @pl.when(n != me)
        def _():
            pl.semaphore_signal(barrier, inc=1, device_id=device_of(n), device_id_type=MESH)
        return carry

    lax.fori_loop(0, n_all, greet, 0)
    grad[...] = jnp.zeros_like(grad)
    loss_acc[...] = jnp.zeros_like(loss_acc)
    tiles[d] = tile_ref[...]
    for c in x_copies:
        c.wait()

    def first(i, carry):
        up_copy(i).wait()
        cols = pl.ds(pl.multiple_of(i * up_w, 128), up_w)
        h = jnp.dot(xs[...], up[:, cols], preferred_element_type=jnp.float32)
        hid[:, cols] = jax.nn.gelu(h).astype(jnp.bfloat16)
        return carry

    lax.fori_loop(0, UP_PARTS, first, 0)

    def second(i, carry):
        down_copy(i).wait()
        cols = pl.ds(pl.multiple_of(i * down_w, 128), down_w)
        part[0, :, cols] = jnp.dot(
            hid[0:own_rows], down[:, cols], preferred_element_type=jnp.float32
        )
        return carry

    lax.fori_loop(0, DOWN_PARTS, second, 0)
    pl.semaphore_wait(barrier, n_all - 1)

    def part_copy(c):
        rows = pl.ds(c * n_rows, n_rows)
        return pltpu.make_async_remote_copy(
            part.at[0, rows], recv.at[rows], part_send.at[c], part_recv.at[c],
            device_id=device(z, y, s, ox), device_id_type=MESH,
        )

    for c in range(n_part):
        part_copy(c).start()

    def tile_copy(n):
        return pltpu.make_async_remote_copy(
            tile_ref, tiles.at[d], tile_send, tile_recv,
            device_id={"dp": n, "section": s, "tensor": x}, device_id_type=MESH,
        )

    def send_tile(n, carry):
        @pl.when(n != d)
        def _():
            tile_copy(n).start()
        return carry

    lax.fori_loop(0, n_dp, send_tile, 0)

    def second_own(i, carry):
        cols = pl.ds(pl.multiple_of(i * down_w, 128), down_w)
        part[1, :, cols] = jnp.dot(
            hid[own_rows:], down[:, cols], preferred_element_type=jnp.float32
        )
        return carry

    lax.fori_loop(0, DOWN_PARTS, second_own, 0)

    def slot(zz, yy, xx):
        return (zz * INNER + yy) * n_tensor + xx

    def place(c, sl):
        return got.at[c, pl.ds(pl.multiple_of(sl * n_rows, n_rows), n_rows)]

    def neighbour(way, ss):
        if way == X:
            return device(z, y, ss, ox)
        if way == Y:
            return device(z, oy, ss, x)
        if way == ZM:
            return device(z - 1, y, ss, x)
        if way == ZP:
            return device(z + 1, y, ss, x)
        return device(z, y, ss, x)

    def own_copy(c, way):
        sl = slot(z, y, x)
        return pltpu.make_async_remote_copy(
            emb.at[pl.ds(c * n_rows, n_rows)], place(c, sl), own_send.at[c, way],
            got_recv.at[c, sl], device_id=neighbour(way, os), device_id_type=MESH,
        )

    def fwd_copy(c, sl, way):
        return pltpu.make_async_remote_copy(
            place(c, sl), place(c, sl), fwd_send.at[c, sl, way], got_recv.at[c, sl],
            device_id=neighbour(way, s), device_id_type=MESH,
        )

    def guarded(way, act):
        if way == ZM:
            pl.when(z > 0)(act)
        elif way == ZP:
            pl.when(z < n_outer - 1)(act)
        else:
            act()

    def own_all(c, begin):
        for way in (ZM, ZP, Y, X, CORE):
            guarded(way, lambda: own_copy(c, way).start() if begin else own_copy(c, way).wait_send())

    def ways(c, rx, ry, far, side):
        onward = ZM if side > 0 else ZP
        if c == 0:
            if far:
                return (onward,)
            return (ZM, ZP) if rx else ((ZM, ZP, X) if ry else ())
        if ry:
            return ()
        if rx:
            return (Y,)
        return (onward, X, Y) if far else ()

    def handle(c, rx, ry, begin, k=0, side=0):
        far = side != 0
        sz = z + side * k
        sl = slot(sz, oy if ry else y, ox if rx else x)

        def act():
            if begin:
                wait_bytes(place(c, sl), got_recv.at[c, sl])
            for way in ways(c, rx, ry, far, side):
                copy = fwd_copy(c, sl, way)
                guarded(way, copy.start if begin else copy.wait_send)

        if far:
            pl.when((sz >= 0) & (sz < n_outer))(act)
        else:
            act()

    def far_loop(begin, blocks):
        def body(k, carry):
            for c, rx, ry in blocks:
                for side in (-1, 1):
                    handle(c, rx, ry, begin, k, side)
            return carry
        lax.fori_loop(1, n_outer, body, 0)

    def produce(c):
        rows = pl.ds(c * n_rows, n_rows)
        part_copy(c).wait_recv()
        raw = (part[1, rows] + recv[rows]) + xs[
            pl.ds(own_rows + c * n_rows, n_rows)
        ].astype(jnp.float32)
        norms = lax.rsqrt(jnp.sum(raw * raw, axis=-1, keepdims=True) + 1e-06)
        emb[rows] = (raw * norms).astype(jnp.bfloat16)
        own_all(c, True)

    others = range(1, n_part)
    near_z = [(c, 0, 0) for c in others] + [(0, 0, 0), (0, 0, 1)]
    far_z = [(0, 1, 0), (0, 1, 1)] + [(c, 1, 0) for c in others]
    scale_value, bias_value = scale_ref[0], bias_ref[0]

    def score(c):
        group = INNER * n_tensor * n_rows

        def body(g, carry):
            block = got[c, pl.ds(pl.multiple_of(g * group, group), group)]
            logits = scale_value * lax.dot_general(
                emb[...], block, (((1,), (1,)), ((), ())), preferred_element_type=jnp.float32
            ) + bias_value
            ids = tiles[g * INNER, c:c + 1]
            for i in range(1, INNER):
                ids = ids + tiles[g * INNER + i, c:c + 1]
            sign = jnp.where(left_ref[...] == ids, 1.0, -1.0).astype(jnp.float32)
            u = -sign * logits
            e = jnp.exp(-jnp.abs(u))
            loss_acc[...] += jnp.maximum(u, 0.0) + jnp.log1p(e)
            sigmoid = jnp.where(u >= 0, 1.0, e) / (1.0 + e)
            weight = (-scale_value * sign * sigmoid).astype(jnp.bfloat16)
            grad[...] += jnp.dot(weight, block, preferred_element_type=jnp.float32)
            return carry

        lax.fori_loop(0, n_outer, body, 0)

    produce(0)
    handle(0, 0, 1, True)
    for c in others:
        produce(c)
    far_loop(True, near_z)
    handle(0, 1, 0, True)
    handle(0, 1, 1, True)
    for c in others:
        handle(c, 1, 0, True)
    far_loop(True, far_z)
    for c in range(n_part):
        handle(c, 0, 0, True)
    wait_bytes(tiles.at[pl.ds(0, n_dp - 1)], tile_recv)
    score(0)
    for c in others:
        handle(c, 0, 1, True)
        handle(c, 1, 1, True)
        far_loop(True, [(c, 0, 1), (c, 1, 1)])
        score(c)

    grad_copy = pltpu.make_async_remote_copy(
        grad.at[pl.ds(pl.multiple_of(os * quarter, 16), quarter)], grad_in, grad_send, grad_recv,
        device_id=device(z, y, os, x), device_id_type=MESH,
    )
    grad_copy.start()
    loss_row[...] = jnp.sum(loss_acc[...], axis=0, keepdims=True)
    loss_all[me] = loss_row[...]

    def loss_copy(n):
        return pltpu.make_async_remote_copy(
            loss_row, loss_all.at[me], loss_send, loss_recv,
            device_id=device_of(n), device_id_type=MESH,
        )

    def send_loss(n, carry):
        @pl.when(n != me)
        def _():
            loss_copy(n).start()
        return carry

    lax.fori_loop(0, n_all, send_loss, 0)

    for c in range(n_part):
        part_copy(c).wait_send()
        own_all(c, False)
    wait_bytes(tiles.at[pl.ds(0, n_dp - 1)], tile_send)
    handle(0, 0, 1, False)
    handle(0, 1, 0, False)
    handle(0, 1, 1, False)
    for c in others:
        handle(c, 1, 0, False)
    far_loop(False, near_z)
    far_loop(False, far_z)

    mine = grad[pl.ds(pl.multiple_of(s * quarter, 16), quarter)]
    grad_copy.wait()

    @pl.when(s == 0)
    def _():
        slide_out[...] = mine
        report_out[...] = grad_in[...]

    @pl.when(s != 0)
    def _():
        slide_out[...] = grad_in[...]
        report_out[...] = mine

    wait_bytes(loss_all.at[pl.ds(0, n_all - 1)], loss_send)
    wait_bytes(loss_all.at[pl.ds(0, n_all - 1)], loss_recv)
    loss_out[0] = jnp.sum(loss_all[...]) * (0.5 / total)


def local(tower_input, up_weight, down_weight, pair, scale, bias):
    n_dp = lax.axis_size("dp")
    n_section = lax.axis_size("section")
    n_tensor = lax.axis_size("tensor")
    d, s, x = lax.axis_index("dp"), lax.axis_index("section"), lax.axis_index("tensor")
    inputs, up_w, down_w = tower_input[0], up_weight[0], down_weight[0]
    rows, width = inputs.shape
    hidden = up_w.shape[1]
    group = n_section * n_tensor
    quarter = rows // group
    own_rows = n_section * quarter
    total = n_dp * rows
    n_rows = 128 // (INNER * n_tensor)
    n_part = own_rows // n_rows
    chips = n_dp * n_tensor

    ids = d * rows + jnp.arange(rows, dtype=jnp.int32)
    left = jnp.where(s == 0, pair, ids).reshape(n_section, n_tensor, quarter)
    left = lax.dynamic_index_in_dim(left, x, 1, keepdims=False).reshape(own_rows, 1)
    left = jnp.broadcast_to(left, (own_rows, 128))
    right = jnp.where(s == 0, ids, pair).reshape(n_section, n_tensor, quarter)
    right = right.transpose(1, 0, 2).reshape(n_tensor, n_part, n_rows)
    right = right.transpose(1, 0, 2).reshape(n_part, 1, n_tensor * n_rows)
    here = jnp.arange(INNER, dtype=jnp.int32)[None, :, None] == lax.rem(d, INNER)
    tile = jnp.where(here, right, 0).reshape(n_part, 128)
    tile = jnp.pad(tile, ((0, 8 - n_part), (0, 0)))

    f32, bf16 = jnp.float32, jnp.bfloat16
    vmem = pl.BlockSpec(memory_space=pltpu.VMEM)
    smem = pl.BlockSpec(memory_space=pltpu.SMEM)
    hbm = pl.BlockSpec(memory_space=pl.ANY)
    dma = pltpu.SemaphoreType.DMA
    n_all = n_dp * group
    dims = (n_dp, n_section, n_tensor, n_part, n_rows, width, total)
    return pl.pallas_call(
        functools.partial(kernel, dims),
        out_shape=(
            jax.ShapeDtypeStruct((1,), f32),
            jax.ShapeDtypeStruct((quarter, width), f32),
            jax.ShapeDtypeStruct((quarter, width), f32),
        ),
        in_specs=[smem, smem, vmem, vmem, hbm, hbm, hbm],
        out_specs=(smem, vmem, vmem),
        scratch_shapes=[
            pltpu.VMEM((rows, width), bf16),
            pltpu.VMEM((width, hidden), bf16),
            pltpu.VMEM((hidden, width), bf16),
            pltpu.VMEM((rows, hidden), bf16),
            pltpu.VMEM((2, own_rows, width), f32),
            pltpu.VMEM((own_rows, width), f32),
            pltpu.VMEM((own_rows, width), bf16),
            pltpu.VMEM((n_part, chips * n_rows, width), bf16),
            pltpu.VMEM((n_dp, 8, 128), jnp.int32),
            pltpu.VMEM((own_rows, width), f32),
            pltpu.VMEM((quarter, width), f32),
            pltpu.VMEM((own_rows, 128), f32),
            pltpu.VMEM((1, 128), f32),
            pltpu.VMEM((n_all, 1, 128), f32),
            dma((group,)),
            dma((UP_PARTS,)),
            dma((DOWN_PARTS,)),
            dma((n_part,)),
            dma((n_part,)),
            dma((n_part, 5)),
            dma((n_part, chips, 4)),
            dma((n_part, chips)),
            dma, dma, dma, dma, dma, dma,
        ],
        compiler_params=pltpu.CompilerParams(
            collective_id=0, has_side_effects=True, vmem_limit_bytes=60 * 1024 * 1024
        ),
    )(scale, bias, left, tile, inputs, up_w, down_w)


def solution(mesh):
    return jax.shard_map(
        local,
        mesh=mesh,
        in_specs=(
            P("section", "dp", None),
            P("section", None, "tensor"),
            P("section", "tensor", None),
            P("dp"),
            P(),
            P(),
        ),
        out_specs=(P(), P(("dp", "section", "tensor"), None), P(("dp", "section", "tensor"), None)),
        check_vma=False,
    )
```

```python
import functools
import math

import jax
import jax.numpy as jnp
from jax import lax
from jax.experimental import pallas as pl
from jax.experimental.pallas import tpu as pltpu
from jax.sharding import PartitionSpec as P

MESH = pl.DeviceIdType.MESH
INNER = 2
UP_PARTS = 4
DOWN_PARTS = 2
X, Y, ZM, ZP, CORE = range(5)
ROUTES = ("zxy", "zxy", "zyx", "yxz", "xzy", "zyx")
N_SUB = len(ROUTES)
ORDER = (
    (0, 0, 0, 0), (1, 0, 0, 0), (0, 0, 0, 1), (2, 0, 0, 0),
    (1, 0, 0, 1), (3, 0, 0, 0), (0, 0, 0, 2), (2, 0, 0, 1),
    (4, 0, 0, 0), (2, 0, 1, 0), (1, 0, 0, 2), (3, 0, 0, 1),
    (5, 0, 0, 0), (0, 1, 0, 0), (3, 0, 1, 0), (0, 0, 0, 3),
    (4, 0, 0, 1), (1, 1, 0, 0), (2, 0, 0, 2), (0, 1, 0, 1),
    (1, 0, 0, 3), (5, 0, 0, 1), (2, 0, 1, 1), (3, 0, 0, 2),
    (1, 1, 0, 1), (3, 0, 1, 1), (5, 0, 1, 0), (3, 1, 0, 0),
    (4, 0, 0, 2), (2, 0, 0, 3), (0, 1, 0, 2), (5, 0, 0, 2),
    (4, 1, 0, 0), (3, 0, 0, 3), (3, 0, 1, 2), (2, 0, 1, 2),
    (1, 1, 0, 2), (4, 0, 0, 3), (3, 1, 0, 1), (0, 1, 0, 3),
    (5, 0, 0, 3), (4, 1, 0, 1), (3, 1, 1, 0), (5, 0, 1, 1),
    (3, 1, 0, 2), (2, 0, 1, 3), (3, 0, 1, 3), (1, 1, 0, 3),
    (4, 1, 0, 2), (3, 1, 0, 3), (3, 1, 1, 1), (5, 0, 1, 2),
    (4, 1, 0, 3), (3, 1, 1, 2), (5, 0, 1, 3), (3, 1, 1, 3),
)


def wait_bytes(ref, sem):
    pltpu.make_async_copy(ref, ref, sem).wait()


def kernel(
    dims,
    scale_ref, bias_ref, pair_ref, x_ref, up_ref, down_ref,
    loss_out, mine_out, theirs_out,
    xs, up, down, hid, part, recv, emb, got, left, tile, tiles, scores, grad, loss_acc, loss_row, loss_all,
    x_sem, up_sem, down_sem, part_send, part_recv, own_send, near_send, fwd_send, got_recv,
    tile_send, tile_recv, grad_send, grad_recv, loss_send, loss_recv,
):
    n_dp, n_section, n_tensor, n_part, n_rows, width, total = dims
    n_outer = n_dp // INNER
    quarter = xs.shape[0] // (n_section * n_tensor)
    own_rows = n_section * quarter
    d, s, x = lax.axis_index("dp"), lax.axis_index("section"), lax.axis_index("tensor")
    z, y = d // INNER, lax.rem(d, INNER)
    ox, oy, os = 1 - x, 1 - y, 1 - s
    n_all = n_dp * n_section * n_tensor
    me = (d * n_section + s) * n_tensor + x

    def device(zz, yy, ss, xx):
        return {"dp": zz * INNER + yy, "section": ss, "tensor": xx}

    def device_of(n):
        return {
            "dp": n // (n_section * n_tensor),
            "section": lax.rem(n // n_tensor, n_section),
            "tensor": lax.rem(n, n_tensor),
        }

    n_sub_rows = own_rows // N_SUB

    def step_of(value, size, count):
        return sum((value >= i * size).astype(jnp.int32) for i in range(1, count))

    def make_ids():
        rows = n_section * n_tensor * quarter
        iota = lambda shape, dim: lax.broadcasted_iota(jnp.int32, shape, dim)
        pair = pair_ref[...].astype(jnp.float32)
        ids = (d * rows + iota((1, rows), 1)).astype(jnp.float32)
        first_core = jnp.broadcast_to(s, (1, rows)) == 0

        def natural(row, t):
            q = step_of(row, quarter, n_section)
            return (q * n_tensor + t) * quarter + (row - q * quarter)

        hit = iota((own_rows, rows), 1) == natural(iota((own_rows, rows), 0), x)
        kept = jnp.sum(jnp.where(hit, jnp.where(first_core, pair, ids), 0.0), axis=1, keepdims=True)
        left[...] = jnp.broadcast_to(kept, (own_rows, 128)).astype(jnp.int32)
        hit = iota((rows, rows), 0) == iota((rows, rows), 1)
        column = jnp.sum(jnp.where(hit, jnp.where(first_core, ids, pair), 0.0), axis=1, keepdims=True)
        lane = iota((rows, 128), 1)
        inner = step_of(lane, n_tensor * n_rows, INNER)
        lane = lane - inner * (n_tensor * n_rows)
        t = step_of(lane, n_rows, n_tensor)
        for c in range(n_part):
            hit = iota((rows, 128), 0) == natural(lane - t * n_rows + c * n_rows, t)
            line = jnp.sum(jnp.where(hit & (inner == y), column, 0.0), axis=0, keepdims=True)
            tile[c:c + 1] = line.astype(jnp.int32)
        tiles[d] = tile[...]

    x_copies = []
    for half, t in ((0, ox), (1, x)):
        for q in range(n_section):
            x_copies.append(pltpu.make_async_copy(
                x_ref.at[pl.ds(pl.multiple_of((q * n_tensor + t) * quarter, 16), quarter)],
                xs.at[pl.ds(half * own_rows + q * quarter, quarter)],
                x_sem.at[half * n_section + q],
            ))
    for c in x_copies:
        c.start()
    up_w = up.shape[1] // UP_PARTS
    down_w = down.shape[1] // DOWN_PARTS

    def up_copy(i):
        cols = pl.ds(pl.multiple_of(i * up_w, 128), up_w)
        return pltpu.make_async_copy(up_ref.at[:, cols], up.at[:, cols], up_sem.at[i])

    def down_copy(i):
        cols = pl.ds(pl.multiple_of(i * down_w, 128), down_w)
        return pltpu.make_async_copy(down_ref.at[:, cols], down.at[:, cols], down_sem.at[i])

    for i in range(UP_PARTS):
        up_copy(i).start()
    for i in range(DOWN_PARTS):
        down_copy(i).start()

    barrier = pltpu.get_barrier_semaphore()

    def greet(n, carry):
        @pl.when(n != me)
        def _():
            pl.semaphore_signal(barrier, inc=1, device_id=device_of(n), device_id_type=MESH)
        return carry

    lax.fori_loop(0, n_all, greet, 0)
    grad[...] = jnp.zeros_like(grad)
    loss_acc[...] = jnp.zeros_like(loss_acc)
    make_ids()
    for c in x_copies:
        c.wait()

    def first(i, carry):
        up_copy(i).wait()
        cols = pl.ds(pl.multiple_of(i * up_w, 128), up_w)
        h = jnp.dot(xs[...], up[:, cols], preferred_element_type=jnp.float32)
        hid[:, cols] = jax.nn.gelu(h).astype(jnp.bfloat16)
        return carry

    lax.fori_loop(0, UP_PARTS, first, 0)

    def second(i, carry):
        down_copy(i).wait()
        cols = pl.ds(pl.multiple_of(i * down_w, 128), down_w)
        part[0, :, cols] = jnp.dot(
            hid[0:own_rows], down[:, cols], preferred_element_type=jnp.float32
        )
        return carry

    lax.fori_loop(0, DOWN_PARTS, second, 0)
    pl.semaphore_wait(barrier, n_all - 1)

    def part_copy(c):
        rows = pl.ds(c * n_sub_rows, n_sub_rows)
        return pltpu.make_async_remote_copy(
            part.at[0, rows], recv.at[rows], part_send.at[c], part_recv.at[c],
            device_id=device(z, y, s, ox), device_id_type=MESH,
        )

    for c in range(N_SUB):
        part_copy(c).start()

    def tile_copy(n):
        return pltpu.make_async_remote_copy(
            tile, tiles.at[d], tile_send, tile_recv,
            device_id={"dp": n, "section": s, "tensor": x}, device_id_type=MESH,
        )

    def send_tile(n, carry):
        @pl.when(n != d)
        def _():
            tile_copy(n).start()
        return carry

    lax.fori_loop(0, n_dp, send_tile, 0)

    def second_own(i, carry):
        cols = pl.ds(pl.multiple_of(i * down_w, 128), down_w)
        part[1, :, cols] = jnp.dot(
            hid[own_rows:], down[:, cols], preferred_element_type=jnp.float32
        )
        return carry

    lax.fori_loop(0, DOWN_PARTS, second_own, 0)

    def slot(zz, yy, xx):
        return (zz * INNER + yy) * n_tensor + xx

    def place(c, sl):
        per = n_rows // n_sub_rows
        start = pl.multiple_of(sl * n_rows + c % per * n_sub_rows, n_sub_rows)
        return got.at[c // per, pl.ds(start, n_sub_rows)]

    def neighbour(way, ss):
        if way == X:
            return device(z, y, ss, ox)
        if way == Y:
            return device(z, oy, ss, x)
        if way == ZM:
            return device(z - 1, y, ss, x)
        if way == ZP:
            return device(z + 1, y, ss, x)
        return device(z, y, ss, x)

    def own_copy(c, way):
        sl = slot(z, y, x)
        return pltpu.make_async_remote_copy(
            emb.at[pl.ds(c * n_sub_rows, n_sub_rows)], place(c, sl), own_send.at[c, way],
            got_recv.at[c, sl], device_id=neighbour(way, os), device_id_type=MESH,
        )

    def fwd_copy(c, sl, way, sem):
        return pltpu.make_async_remote_copy(
            place(c, sl), place(c, sl), sem, got_recv.at[c, sl],
            device_id=neighbour(way, s), device_id_type=MESH,
        )

    def guarded(way, act):
        if way == ZM:
            pl.when(z > 0)(act)
        elif way == ZP:
            pl.when(z < n_outer - 1)(act)
        else:
            act()

    def own_all(c, begin):
        for way in (ZM, ZP, Y, X, CORE):
            guarded(way, lambda: own_copy(c, way).start() if begin else own_copy(c, way).wait_send())

    def ways(c, rx, ry, far, side):
        moved = {"x": rx, "y": ry, "z": far}
        route = ROUTES[c]
        done = max((i + 1 for i in range(3) if moved[route[i]]), default=0)
        if not done:
            return ()
        out = {"x": (X,), "y": (Y,), "z": (ZM, ZP)}
        onward = (ZM if side > 0 else ZP,) if route[done - 1] == "z" else ()
        return sum((out[i] for i in route[done:]), onward)

    def handle(c, rx, ry, begin, k=0, side=0):
        far = side != 0
        sz = z + side * k
        sl = slot(sz, oy if ry else y, ox if rx else x)

        def act():
            if begin:
                wait_bytes(place(c, sl), got_recv.at[c, sl])
            for way in ways(c, rx, ry, far, side):
                if way == ZP and not far:
                    sem = near_send.at[c, rx * INNER + ry]
                else:
                    sem = fwd_send.at[c, sl, min(way, ZM)]
                copy = fwd_copy(c, sl, way, sem)
                guarded(way, copy.start if begin else copy.wait_send)

        if far:
            pl.when((sz >= 0) & (sz < n_outer))(act)
        else:
            act()

    def far_loop(begin, blocks):
        def body(k, carry):
            for c, rx, ry in blocks:
                for side in (-1, 1):
                    handle(c, rx, ry, begin, k, side)
            return carry
        lax.fori_loop(1, n_outer, body, 0)

    def produce(c):
        rows = pl.ds(c * n_sub_rows, n_sub_rows)
        part_copy(c).wait_recv()
        raw = (part[1, rows] + recv[rows]) + xs[
            pl.ds(own_rows + c * n_sub_rows, n_sub_rows)
        ].astype(jnp.float32)
        norms = lax.rsqrt(jnp.sum(raw * raw, axis=-1, keepdims=True) + 1e-06)
        emb[rows] = (raw * norms).astype(jnp.bfloat16)
        own_all(c, True)

    scale_value, bias_value = scale_ref[0], bias_ref[0]
    batch = math.gcd(4, n_outer)
    group = batch * INNER * n_tensor * n_rows
    group_lanes = lambda g: pl.ds(pl.multiple_of(g * group, 128), group)

    def score(c):
        def body(g, carry):
            block = got[c, pl.ds(pl.multiple_of(g * group, group), group)]
            logits = scale_value * lax.dot_general(
                emb[...], block, (((1,), (1,)), ((), ())), preferred_element_type=jnp.float32
            ) + bias_value
            lines = []
            for j in range(batch):
                at = (g * batch + j) * INNER
                lines.append(sum(tiles[at + i, c:c + 1] for i in range(INNER)))
            for j in range(batch):
                sign = jnp.where(left[...] == lines[j], 1.0, -1.0).astype(jnp.float32)
                u = -sign * logits[:, j * 128:(j + 1) * 128]
                e = jnp.exp(-jnp.abs(u))
                loss_acc[...] += jnp.maximum(u, 0.0) + jnp.log1p(e)
                sigmoid = jnp.where(u >= 0, 1.0, e) / (1.0 + e)
                lanes = pl.ds(pl.multiple_of(g * group + j * 128, 128), 128)
                scores[:, lanes] = (-scale_value * sign * sigmoid).astype(jnp.bfloat16)
            return carry

        lax.fori_loop(0, n_outer // batch, body, 0)

    def collect(c):
        def body(g, carry):
            block = got[c, pl.ds(pl.multiple_of(g * group, group), group)]
            grad[...] += jnp.dot(
                scores[:, group_lanes(g)], block, preferred_element_type=jnp.float32
            )
            return carry

        lax.fori_loop(0, n_outer // batch, body, 0)

    shifts = [(c, rx, ry) for c in range(N_SUB) for rx in (0, 1) for ry in (0, 1)]
    passed = [b for b in sorted(shifts, key=lambda b: b[1] + b[2]) if ways(*b, True, 1)]
    table_k = max(k for _, _, _, k in ORDER)

    def pass_on(begin):
        for c, rx, ry, k in ORDER:
            if k >= n_outer:
                continue
            if k:
                for side in (-1, 1):
                    handle(c, rx, ry, begin, k, side)
            elif rx or ry:
                handle(c, rx, ry, begin)
            elif begin:
                produce(c)
            else:
                own_all(c, False)

        def body(k, carry):
            for c, rx, ry in passed:
                for side in (-1, 1):
                    handle(c, rx, ry, begin, k, side)
            return carry

        if table_k + 1 < n_outer:
            lax.fori_loop(table_k + 1, n_outer, body, 0)

    def finish(c):
        per = n_rows // n_sub_rows
        blocks = [b for b in shifts if b[0] // per == c]
        for b in blocks:
            if b[1:] == (0, 0) or not ways(*b, False, 0):
                handle(*b, True)
        ends = [b for b in blocks if not ways(*b, True, 1)]

        def body(k, carry):
            for b in ends:
                for side in (-1, 1):
                    handle(*b, True, k, side)
            return carry

        lax.fori_loop(1, n_outer, body, 0)

    pass_on(True)
    wait_bytes(tiles.at[pl.ds(0, n_dp - 1)], tile_recv)

    def loss_copy(n):
        return pltpu.make_async_remote_copy(
            loss_row, loss_all.at[me], loss_send, loss_recv,
            device_id=device_of(n), device_id_type=MESH,
        )

    def send_loss(n, carry):
        @pl.when(n != me)
        def _():
            loss_copy(n).start()
        return carry

    for c in range(n_part):
        finish(c)
        score(c)
        if c == n_part - 1:
            loss_row[...] = jnp.sum(loss_acc[...], axis=0, keepdims=True)
            loss_all[me] = loss_row[...]
            lax.fori_loop(0, n_all, send_loss, 0)
        collect(c)

    grad_copy = pltpu.make_async_remote_copy(
        grad.at[pl.ds(pl.multiple_of(os * quarter, 16), quarter)], theirs_out, grad_send, grad_recv,
        device_id=device(z, y, os, x), device_id_type=MESH,
    )
    grad_copy.start()
    mine_out[...] = grad[pl.ds(pl.multiple_of(s * quarter, 16), quarter)]
    for c in range(N_SUB):
        part_copy(c).wait_send()
    wait_bytes(tiles.at[pl.ds(0, n_dp - 1)], tile_send)
    pass_on(False)
    grad_copy.wait()
    wait_bytes(loss_all.at[pl.ds(0, n_all - 1)], loss_send)
    wait_bytes(loss_all.at[pl.ds(0, n_all - 1)], loss_recv)
    loss_out[0] = jnp.sum(loss_all[...]) * (0.5 / total)


def local(tower_input, up_weight, down_weight, pair, scale, bias):
    n_dp = lax.axis_size("dp")
    n_section = lax.axis_size("section")
    n_tensor = lax.axis_size("tensor")
    inputs, up_w, down_w = tower_input[0], up_weight[0], down_weight[0]
    rows, width = inputs.shape
    hidden = up_w.shape[1]
    group = n_section * n_tensor
    quarter = rows // group
    own_rows = n_section * quarter
    total = n_dp * rows
    n_rows = 128 // (INNER * n_tensor)
    n_part = own_rows // n_rows
    chips = n_dp * n_tensor

    f32, bf16 = jnp.float32, jnp.bfloat16
    vmem = pl.BlockSpec(memory_space=pltpu.VMEM)
    smem = pl.BlockSpec(memory_space=pltpu.SMEM)
    hbm = pl.BlockSpec(memory_space=pl.ANY)
    dma = pltpu.SemaphoreType.DMA
    n_all = n_dp * group
    dims = (n_dp, n_section, n_tensor, n_part, n_rows, width, total)
    loss, mine, theirs = pl.pallas_call(
        functools.partial(kernel, dims),
        out_shape=(
            jax.ShapeDtypeStruct((1,), f32),
            jax.ShapeDtypeStruct((quarter, width), f32),
            jax.ShapeDtypeStruct((quarter, width), f32),
        ),
        in_specs=[smem, smem, vmem, hbm, hbm, hbm],
        out_specs=(smem, vmem, vmem),
        scratch_shapes=[
            pltpu.VMEM((rows, width), bf16),
            pltpu.VMEM((width, hidden), bf16),
            pltpu.VMEM((hidden, width), bf16),
            pltpu.VMEM((rows, hidden), bf16),
            pltpu.VMEM((2, own_rows, width), f32),
            pltpu.VMEM((own_rows, width), f32),
            pltpu.VMEM((own_rows, width), bf16),
            pltpu.VMEM((n_part, chips * n_rows, width), bf16),
            pltpu.VMEM((own_rows, 128), jnp.int32),
            pltpu.VMEM((8, 128), jnp.int32),
            pltpu.VMEM((n_dp, 8, 128), jnp.int32),
            pltpu.VMEM((own_rows, chips * n_rows), bf16),
            pltpu.VMEM((own_rows, width), f32),
            pltpu.VMEM((own_rows, 128), f32),
            pltpu.VMEM((1, 128), f32),
            pltpu.VMEM((n_all, 1, 128), f32),
            dma((group,)),
            dma((UP_PARTS,)),
            dma((DOWN_PARTS,)),
            dma((N_SUB,)),
            dma((N_SUB,)),
            dma((N_SUB, 5)),
            dma((N_SUB, n_tensor * INNER)),
            dma((N_SUB, chips, 3)),
            dma((N_SUB, chips)),
            dma, dma, dma, dma, dma, dma,
        ],
        compiler_params=pltpu.CompilerParams(
            collective_id=0, has_side_effects=True, vmem_limit_bytes=60 * 1024 * 1024
        ),
    )(scale, bias, pair.reshape(1, rows), inputs, up_w, down_w)
    first_core = lax.axis_index("section") == 0
    return (
        loss,
        jnp.where(first_core, mine, theirs),
        jnp.where(first_core, theirs, mine),
    )


def solution(mesh):
    return jax.shard_map(
        local,
        mesh=mesh,
        in_specs=(
            P("section", "dp", None),
            P("section", None, "tensor"),
            P("section", "tensor", None),
            P("dp"),
            P(),
            P(),
        ),
        out_specs=(P(), P(("dp", "section", "tensor"), None), P(("dp", "section", "tensor"), None)),
        check_vma=False,
    )
```

```python
import functools
import math

import jax
import jax.numpy as jnp
from jax import lax
from jax.experimental import pallas as pl
from jax.experimental.pallas import tpu as pltpu
from jax.sharding import PartitionSpec as P

MESH = pl.DeviceIdType.MESH
INNER = 2
UP_PARTS = 4
DOWN_PARTS = 2
X, Y, ZM, ZP, CORE = range(5)
ROUTES = ("zxy", "zxy", "zyx", "yxz", "xzy", "zyx")
N_SUB = len(ROUTES)
ORDER = (
    (0, 0, 0, 0), (1, 0, 0, 0), (0, 0, 0, 1), (2, 0, 0, 0),
    (1, 0, 0, 1), (3, 0, 0, 0), (0, 0, 0, 2), (2, 0, 0, 1),
    (4, 0, 0, 0), (2, 0, 1, 0), (1, 0, 0, 2), (3, 0, 0, 1),
    (5, 0, 0, 0), (0, 1, 0, 0), (3, 0, 1, 0), (0, 0, 0, 3),
    (4, 0, 0, 1), (1, 1, 0, 0), (2, 0, 0, 2), (0, 1, 0, 1),
    (1, 0, 0, 3), (5, 0, 0, 1), (2, 0, 1, 1), (3, 0, 0, 2),
    (1, 1, 0, 1), (3, 0, 1, 1), (5, 0, 1, 0), (3, 1, 0, 0),
    (4, 0, 0, 2), (2, 0, 0, 3), (0, 1, 0, 2), (5, 0, 0, 2),
    (4, 1, 0, 0), (3, 0, 0, 3), (3, 0, 1, 2), (2, 0, 1, 2),
    (1, 1, 0, 2), (4, 0, 0, 3), (3, 1, 0, 1), (0, 1, 0, 3),
    (5, 0, 0, 3), (4, 1, 0, 1), (3, 1, 1, 0), (5, 0, 1, 1),
    (3, 1, 0, 2), (2, 0, 1, 3), (3, 0, 1, 3), (1, 1, 0, 3),
    (4, 1, 0, 2), (3, 1, 0, 3), (3, 1, 1, 1), (5, 0, 1, 2),
    (4, 1, 0, 3), (3, 1, 1, 2), (5, 0, 1, 3), (3, 1, 1, 3),
)


def wait_bytes(ref, sem):
    pltpu.make_async_copy(ref, ref, sem).wait()


def kernel(
    dims,
    scale_ref, bias_ref, pair_ref, x_ref, up_ref, down_ref,
    loss_out, mine_out, theirs_out,
    xs, up, down, hid, part, recv, emb, got, left, tile, tiles, scores, grad, loss_acc, loss_row, loss_all,
    x_sem, up_sem, down_sem, part_send, part_recv, own_send, near_send, fwd_send, got_recv,
    tile_send, tile_recv, grad_send, grad_recv, loss_send, loss_recv,
):
    n_dp, n_section, n_tensor, n_part, n_rows, width, total = dims
    n_outer = n_dp // INNER
    quarter = xs.shape[0] // (n_section * n_tensor)
    own_rows = n_section * quarter
    d, s, x = lax.axis_index("dp"), lax.axis_index("section"), lax.axis_index("tensor")
    z, y = d // INNER, lax.rem(d, INNER)
    ox, oy, os = 1 - x, 1 - y, 1 - s
    n_all = n_dp * n_section * n_tensor
    me = (d * n_section + s) * n_tensor + x

    def device(zz, yy, ss, xx):
        return {"dp": zz * INNER + yy, "section": ss, "tensor": xx}

    def device_of(n):
        return {
            "dp": n // (n_section * n_tensor),
            "section": lax.rem(n // n_tensor, n_section),
            "tensor": lax.rem(n, n_tensor),
        }

    n_sub_rows = own_rows // N_SUB

    def step_of(value, size, count):
        return sum((value >= i * size).astype(jnp.int32) for i in range(1, count))

    def make_ids():
        rows = n_section * n_tensor * quarter
        iota = lambda shape, dim: lax.broadcasted_iota(jnp.int32, shape, dim)
        pair = pair_ref[...].astype(jnp.float32)
        ids = (d * rows + iota((1, rows), 1)).astype(jnp.float32)
        first_core = jnp.broadcast_to(s, (1, rows)) == 0

        def natural(row, t):
            q = step_of(row, quarter, n_section)
            return (q * n_tensor + t) * quarter + (row - q * quarter)

        hit = iota((own_rows, rows), 1) == natural(iota((own_rows, rows), 0), x)
        kept = jnp.sum(jnp.where(hit, jnp.where(first_core, pair, ids), 0.0), axis=1, keepdims=True)
        left[...] = jnp.broadcast_to(kept, (own_rows, 128)).astype(jnp.int32)
        hit = iota((rows, rows), 0) == iota((rows, rows), 1)
        column = jnp.sum(jnp.where(hit, jnp.where(first_core, ids, pair), 0.0), axis=1, keepdims=True)
        lane = iota((rows, 128), 1)
        inner = step_of(lane, n_tensor * n_rows, INNER)
        lane = lane - inner * (n_tensor * n_rows)
        t = step_of(lane, n_rows, n_tensor)
        for c in range(n_part):
            hit = iota((rows, 128), 0) == natural(lane - t * n_rows + c * n_rows, t)
            line = jnp.sum(jnp.where(hit & (inner == y), column, 0.0), axis=0, keepdims=True)
            tile[c:c + 1] = line.astype(jnp.int32)
        tiles[d] = tile[...]

    x_copies = []
    for half, t in ((0, ox), (1, x)):
        for q in range(n_section):
            x_copies.append(pltpu.make_async_copy(
                x_ref.at[pl.ds(pl.multiple_of((q * n_tensor + t) * quarter, 16), quarter)],
                xs.at[pl.ds(half * own_rows + q * quarter, quarter)],
                x_sem.at[half * n_section + q],
            ))
    for c in x_copies:
        c.start()
    up_w = up.shape[1] // UP_PARTS
    down_w = down.shape[1] // DOWN_PARTS

    def up_copy(i):
        cols = pl.ds(pl.multiple_of(i * up_w, 128), up_w)
        return pltpu.make_async_copy(up_ref.at[:, cols], up.at[:, cols], up_sem.at[i])

    def down_copy(i):
        cols = pl.ds(pl.multiple_of(i * down_w, 128), down_w)
        return pltpu.make_async_copy(down_ref.at[:, cols], down.at[:, cols], down_sem.at[i])

    for i in range(UP_PARTS):
        up_copy(i).start()
    for i in range(DOWN_PARTS):
        down_copy(i).start()

    barrier = pltpu.get_barrier_semaphore()

    def greet(n, carry):
        @pl.when(n != me)
        def _():
            pl.semaphore_signal(barrier, inc=1, device_id=device_of(n), device_id_type=MESH)
        return carry

    lax.fori_loop(0, n_all, greet, 0)
    grad[...] = jnp.zeros_like(grad)
    loss_acc[...] = jnp.zeros_like(loss_acc)
    make_ids()
    for c in x_copies:
        c.wait()

    def first(half):
        rows = pl.ds(half * own_rows, own_rows)

        def body(i, carry):
            if half == 0:
                up_copy(i).wait()
            cols = pl.ds(pl.multiple_of(i * up_w, 128), up_w)
            h = jnp.dot(xs[rows], up[:, cols], preferred_element_type=jnp.float32)
            hid[rows, cols] = jax.nn.gelu(h).astype(jnp.bfloat16)
            return carry

        lax.fori_loop(0, UP_PARTS, body, 0)

    first(0)

    def second(i, carry):
        down_copy(i).wait()
        cols = pl.ds(pl.multiple_of(i * down_w, 128), down_w)
        part[0, :, cols] = jnp.dot(
            hid[0:own_rows], down[:, cols], preferred_element_type=jnp.float32
        )
        return carry

    lax.fori_loop(0, DOWN_PARTS, second, 0)
    pl.semaphore_wait(barrier, n_all - 1)

    def part_copy(c):
        rows = pl.ds(c * n_sub_rows, n_sub_rows)
        return pltpu.make_async_remote_copy(
            part.at[0, rows], recv.at[rows], part_send.at[c], part_recv.at[c],
            device_id=device(z, y, s, ox), device_id_type=MESH,
        )

    for c in range(N_SUB):
        part_copy(c).start()

    def tile_copy(n):
        return pltpu.make_async_remote_copy(
            tile, tiles.at[d], tile_send, tile_recv,
            device_id={"dp": n, "section": s, "tensor": x}, device_id_type=MESH,
        )

    def send_tile(n, carry):
        @pl.when(n != d)
        def _():
            tile_copy(n).start()
        return carry

    lax.fori_loop(0, n_dp, send_tile, 0)

    first(1)

    def second_own(i, carry):
        cols = pl.ds(pl.multiple_of(i * down_w, 128), down_w)
        part[1, :, cols] = jnp.dot(
            hid[own_rows:], down[:, cols], preferred_element_type=jnp.float32
        )
        return carry

    lax.fori_loop(0, DOWN_PARTS, second_own, 0)

    def slot(zz, yy, xx):
        return (zz * INNER + yy) * n_tensor + xx

    def place(c, sl):
        per = n_rows // n_sub_rows
        start = pl.multiple_of(sl * n_rows + c % per * n_sub_rows, n_sub_rows)
        return got.at[c // per, pl.ds(start, n_sub_rows)]

    def neighbour(way, ss):
        if way == X:
            return device(z, y, ss, ox)
        if way == Y:
            return device(z, oy, ss, x)
        if way == ZM:
            return device(z - 1, y, ss, x)
        if way == ZP:
            return device(z + 1, y, ss, x)
        return device(z, y, ss, x)

    def own_copy(c, way):
        sl = slot(z, y, x)
        return pltpu.make_async_remote_copy(
            emb.at[pl.ds(c * n_sub_rows, n_sub_rows)], place(c, sl), own_send.at[c, way],
            got_recv.at[c, sl], device_id=neighbour(way, os), device_id_type=MESH,
        )

    def fwd_copy(c, sl, way, sem):
        return pltpu.make_async_remote_copy(
            place(c, sl), place(c, sl), sem, got_recv.at[c, sl],
            device_id=neighbour(way, s), device_id_type=MESH,
        )

    def guarded(way, act):
        if way == ZM:
            pl.when(z > 0)(act)
        elif way == ZP:
            pl.when(z < n_outer - 1)(act)
        else:
            act()

    def own_all(c, begin):
        for way in (ZM, ZP, Y, X, CORE):
            guarded(way, lambda: own_copy(c, way).start() if begin else own_copy(c, way).wait_send())

    def ways(c, rx, ry, far, side):
        moved = {"x": rx, "y": ry, "z": far}
        route = ROUTES[c]
        done = max((i + 1 for i in range(3) if moved[route[i]]), default=0)
        if not done:
            return ()
        out = {"x": (X,), "y": (Y,), "z": (ZM, ZP)}
        onward = (ZM if side > 0 else ZP,) if route[done - 1] == "z" else ()
        return sum((out[i] for i in route[done:]), onward)

    def handle(c, rx, ry, begin, k=0, side=0):
        far = side != 0
        sz = z + side * k
        sl = slot(sz, oy if ry else y, ox if rx else x)

        def act():
            if begin:
                wait_bytes(place(c, sl), got_recv.at[c, sl])
            for way in ways(c, rx, ry, far, side):
                if way == ZP and not far:
                    sem = near_send.at[c, rx * INNER + ry]
                else:
                    sem = fwd_send.at[c, sl, min(way, ZM)]
                copy = fwd_copy(c, sl, way, sem)
                guarded(way, copy.start if begin else copy.wait_send)

        if far:
            pl.when((sz >= 0) & (sz < n_outer))(act)
        else:
            act()

    def far_loop(begin, blocks):
        def body(k, carry):
            for c, rx, ry in blocks:
                for side in (-1, 1):
                    handle(c, rx, ry, begin, k, side)
            return carry
        lax.fori_loop(1, n_outer, body, 0)

    def produce(c):
        rows = pl.ds(c * n_sub_rows, n_sub_rows)
        part_copy(c).wait_recv()
        raw = (part[1, rows] + recv[rows]) + xs[
            pl.ds(own_rows + c * n_sub_rows, n_sub_rows)
        ].astype(jnp.float32)
        norms = lax.rsqrt(jnp.sum(raw * raw, axis=-1, keepdims=True) + 1e-06)
        emb[rows] = (raw * norms).astype(jnp.bfloat16)
        own_all(c, True)

    scale_value, bias_value = scale_ref[0], bias_ref[0]
    batch = math.gcd(4, n_outer)
    group = batch * INNER * n_tensor * n_rows
    group_lanes = lambda g: pl.ds(pl.multiple_of(g * group, 128), group)

    def score(c):
        def body(g, carry):
            block = got[c, pl.ds(pl.multiple_of(g * group, group), group)]
            logits = scale_value * lax.dot_general(
                emb[...], block, (((1,), (1,)), ((), ())), preferred_element_type=jnp.float32
            ) + bias_value
            lines = []
            for j in range(batch):
                at = (g * batch + j) * INNER
                lines.append(sum(tiles[at + i, c:c + 1] for i in range(INNER)))
            for j in range(batch):
                sign = jnp.where(left[...] == lines[j], 1.0, -1.0).astype(jnp.float32)
                u = -sign * logits[:, j * 128:(j + 1) * 128]
                e = jnp.exp(-jnp.abs(u))
                loss_acc[...] += jnp.maximum(u, 0.0) + jnp.log1p(e)
                sigmoid = jnp.where(u >= 0, 1.0, e) / (1.0 + e)
                lanes = pl.ds(pl.multiple_of(g * group + j * 128, 128), 128)
                scores[:, lanes] = (-scale_value * sign * sigmoid).astype(jnp.bfloat16)
            return carry

        lax.fori_loop(0, n_outer // batch, body, 0)

    def collect(c):
        def body(g, carry):
            block = got[c, pl.ds(pl.multiple_of(g * group, group), group)]
            grad[...] += jnp.dot(
                scores[:, group_lanes(g)], block, preferred_element_type=jnp.float32
            )
            return carry

        lax.fori_loop(0, n_outer // batch, body, 0)

    shifts = [(c, rx, ry) for c in range(N_SUB) for rx in (0, 1) for ry in (0, 1)]
    passed = [b for b in sorted(shifts, key=lambda b: b[1] + b[2]) if ways(*b, True, 1)]
    table_k = max(k for _, _, _, k in ORDER)

    def pass_on(begin):
        for c, rx, ry, k in ORDER:
            if k >= n_outer:
                continue
            if k:
                for side in (-1, 1):
                    handle(c, rx, ry, begin, k, side)
            elif rx or ry:
                handle(c, rx, ry, begin)
            elif begin:
                produce(c)
            else:
                own_all(c, False)

        def body(k, carry):
            for c, rx, ry in passed:
                for side in (-1, 1):
                    handle(c, rx, ry, begin, k, side)
            return carry

        if table_k + 1 < n_outer:
            lax.fori_loop(table_k + 1, n_outer, body, 0)

    def finish(c):
        per = n_rows // n_sub_rows
        blocks = [b for b in shifts if b[0] // per == c]
        for b in blocks:
            if b[1:] == (0, 0) or not ways(*b, False, 0):
                handle(*b, True)
        ends = [b for b in blocks if not ways(*b, True, 1)]

        def body(k, carry):
            for b in ends:
                for side in (-1, 1):
                    handle(*b, True, k, side)
            return carry

        lax.fori_loop(1, n_outer, body, 0)

    pass_on(True)
    wait_bytes(tiles.at[pl.ds(0, n_dp - 1)], tile_recv)

    def loss_copy(n):
        return pltpu.make_async_remote_copy(
            loss_row, loss_all.at[slot(z, y, x)], loss_send, loss_recv,
            device_id=device_of(n), device_id_type=MESH,
        )

    def send_loss(n, carry):
        loss_copy(lax.rem(me + n, n_all)).start()
        return carry

    for c in range(n_part):
        finish(c)
        score(c)
        if c == n_part - 1:
            loss_row[...] = jnp.sum(loss_acc[...], axis=0, keepdims=True)

            @pl.when(s == 0)
            def _():
                loss_all[slot(z, y, x)] = loss_row[...]
                lax.fori_loop(1, n_all, send_loss, 0)

        collect(c)

    grad_copy = pltpu.make_async_remote_copy(
        grad.at[pl.ds(pl.multiple_of(os * quarter, 16), quarter)], theirs_out, grad_send, grad_recv,
        device_id=device(z, y, os, x), device_id_type=MESH,
    )
    grad_copy.start()
    mine_out[...] = grad[pl.ds(pl.multiple_of(s * quarter, 16), quarter)]
    for c in range(N_SUB):
        part_copy(c).wait_send()
    wait_bytes(tiles.at[pl.ds(0, n_dp - 1)], tile_send)
    pass_on(False)
    grad_copy.wait()
    n_chips = n_dp * n_tensor

    @pl.when(s == 0)
    def _():
        wait_bytes(loss_all.at[pl.ds(0, n_all - 1)], loss_send)
        wait_bytes(loss_all.at[pl.ds(0, n_chips - 1)], loss_recv)

    @pl.when(s != 0)
    def _():
        wait_bytes(loss_all.at[pl.ds(0, n_chips)], loss_recv)

    loss_out[0] = jnp.sum(loss_all[0:n_chips]) / total


def local(tower_input, up_weight, down_weight, pair, scale, bias):
    n_dp = lax.axis_size("dp")
    n_section = lax.axis_size("section")
    n_tensor = lax.axis_size("tensor")
    inputs, up_w, down_w = tower_input[0], up_weight[0], down_weight[0]
    rows, width = inputs.shape
    hidden = up_w.shape[1]
    group = n_section * n_tensor
    quarter = rows // group
    own_rows = n_section * quarter
    total = n_dp * rows
    n_rows = 128 // (INNER * n_tensor)
    n_part = own_rows // n_rows
    chips = n_dp * n_tensor

    f32, bf16 = jnp.float32, jnp.bfloat16
    vmem = pl.BlockSpec(memory_space=pltpu.VMEM)
    smem = pl.BlockSpec(memory_space=pltpu.SMEM)
    hbm = pl.BlockSpec(memory_space=pl.ANY)
    dma = pltpu.SemaphoreType.DMA
    n_all = n_dp * group
    dims = (n_dp, n_section, n_tensor, n_part, n_rows, width, total)
    loss, mine, theirs = pl.pallas_call(
        functools.partial(kernel, dims),
        out_shape=(
            jax.ShapeDtypeStruct((1,), f32),
            jax.ShapeDtypeStruct((quarter, width), f32),
            jax.ShapeDtypeStruct((quarter, width), f32),
        ),
        in_specs=[smem, smem, vmem, hbm, hbm, hbm],
        out_specs=(smem, vmem, vmem),
        scratch_shapes=[
            pltpu.VMEM((rows, width), bf16),
            pltpu.VMEM((width, hidden), bf16),
            pltpu.VMEM((hidden, width), bf16),
            pltpu.VMEM((rows, hidden), bf16),
            pltpu.VMEM((2, own_rows, width), f32),
            pltpu.VMEM((own_rows, width), f32),
            pltpu.VMEM((own_rows, width), bf16),
            pltpu.VMEM((n_part, chips * n_rows, width), bf16),
            pltpu.VMEM((own_rows, 128), jnp.int32),
            pltpu.VMEM((8, 128), jnp.int32),
            pltpu.VMEM((n_dp, 8, 128), jnp.int32),
            pltpu.VMEM((own_rows, chips * n_rows), bf16),
            pltpu.VMEM((own_rows, width), f32),
            pltpu.VMEM((own_rows, 128), f32),
            pltpu.VMEM((1, 128), f32),
            pltpu.VMEM((n_all, 1, 128), f32),
            dma((group,)),
            dma((UP_PARTS,)),
            dma((DOWN_PARTS,)),
            dma((N_SUB,)),
            dma((N_SUB,)),
            dma((N_SUB, 5)),
            dma((N_SUB, n_tensor * INNER)),
            dma((N_SUB, chips, 3)),
            dma((N_SUB, chips)),
            dma, dma, dma, dma, dma, dma,
        ],
        compiler_params=pltpu.CompilerParams(
            collective_id=0, has_side_effects=True, vmem_limit_bytes=60 * 1024 * 1024
        ),
    )(scale, bias, pair.reshape(1, rows), inputs, up_w, down_w)
    first_core = lax.axis_index("section") == 0
    return (
        loss,
        jnp.where(first_core, mine, theirs),
        jnp.where(first_core, theirs, mine),
    )


def solution(mesh):
    return jax.shard_map(
        local,
        mesh=mesh,
        in_specs=(
            P("section", "dp", None),
            P("section", None, "tensor"),
            P("section", "tensor", None),
            P("dp"),
            P(),
            P(),
        ),
        out_specs=(P(), P(("dp", "section", "tensor"), None), P(("dp", "section", "tensor"), None)),
        check_vma=False,
    )
```
